32 devices in a mesh: row: 16 (over z, y, core), col: 2 (over x).
Axes of the slice: x: 2, y: 2, z: 4, core: 2. Of those that a mesh axis runs over, the one named last changes fastest.
Arguments:
- eigvec: float32 [65536, 1024], P('row', 'col'), may hold values from -6 to 6
- reflectors: float32 [16, 2, 1024, 256], P('row', 'col'), may hold values from -0.125 to 0.125
- tfactors: float32 [16, 2, 256, 256], P('row', 'col'), may hold values from -1 to 1, as said below
- offsets: int32 [2, 16], replicated, may hold values from 3072 to 3584
- owners: int32 [2, 16], replicated, may hold values from 0 to 1
Outputs:
- result: float32 [65536, 1024], P('row', 'col')
The draws below stay inside these ranges and needn't reach their ends.
Inputs may be any that keep to these rules, and one draw needn't show every extreme that they name: `tfactors`: every factor block is zero below its diagonal.
All inputs are finite; a program needn't handle non-finite values.
Results may differ from the reference program's by a relative error of at most 0.0003.
Values sent between devices are 32-bit elements; how exact they have to be, the bound alone decides.
A program may use at most 64 MiB of HBM per device.

```python
import jax
import jax.numpy as jnp
from jax import lax

ORDER = 65536
WIN = 1024
BLOCK = 256
TICKS = 2
HALF = 512
ROWS_DEV = 4096
NCOLS = 1024
N_ROW = 16
N_COL = 2


def draw_tfactors(key, part):
    key_diag, key_upper = jax.random.split(jax.random.fold_in(key, 11))
    diagonal = jax.random.uniform(key_diag, (N_ROW, N_COL, BLOCK), jnp.float32, 0.3, 1.0)
    off_scale = 0.6
    entries = jax.random.normal(key_upper, (N_ROW, N_COL, BLOCK, BLOCK), jnp.float32) * (off_scale / BLOCK ** 0.5)
    positions = jnp.arange(BLOCK)
    strict_mask = positions[:, None] < positions[None, :]
    identity = (positions[:, None] == positions[None, :]).astype(jnp.float32)
    return jnp.where(strict_mask, entries, 0.0) + diagonal[..., None] * identity


def plant(result, rng, smallest, top_value):
    longest = result.shape.index(max(result.shape))
    spots = []
    for shift in (0, 1):
        where = [jax.random.randint(jax.random.fold_in(rng, axis), (), 0, length) for axis, length in enumerate(result.shape)]
        where[longest] = (where[longest] + shift) % result.shape[longest]
        spots.append(tuple(where))
    return result.at[spots[0]].set(smallest).at[spots[1]].set(top_value)


def steps_of(own_key, extent, cuts, least, high):
    loudness, own = 1.0, jax.random.fold_in(own_key, 6)
    for dim, parts in cuts:
        draws = jnp.exp(jax.random.uniform(jax.random.fold_in(own, dim), (parts,), jnp.float32, least / len(cuts), high / len(cuts)))
        loudness = loudness * jnp.repeat(draws, extent[dim] // parts).reshape([-1 if axis == dim else 1 for axis in range(len(extent))])
    return loudness


def bell_draw(stream_key, extent, scale, most, cuts=(), kind=jnp.bfloat16):
    level = steps_of(stream_key, extent, cuts, -0.22, 0.18) if cuts else 1.0
    array = jax.random.normal(stream_key, extent, jnp.float32) * scale * level
    return jnp.minimum(jnp.maximum(array, -most), most).astype(kind)


def setup_inputs(seed: int = 0) -> dict:
    key_of = jax.random.split(jax.random.key(seed), 6)
    return {
        "eigvec": bell_draw(key_of[0], (ORDER, NCOLS), 1.0, 6.0, ((0, 16), (1, 2)), jnp.float32),
        "reflectors": bell_draw(key_of[1], (N_ROW, N_COL, WIN, BLOCK), (2 * WIN) ** -0.5, 0.125, ((0, 16), (1, 2)), jnp.float32),
        "tfactors": draw_tfactors(jax.random.fold_in(key_of[5], 71), 0),
        "offsets": plant(jax.random.randint(key_of[3], (TICKS, N_ROW), ROWS_DEV - WIN, ROWS_DEV - HALF + 1), jax.random.fold_in(key_of[3], 1), ROWS_DEV - WIN, ROWS_DEV - HALF).astype(jnp.int32),
        "owners": plant(jax.random.randint(key_of[4], (TICKS, N_ROW), 0, N_COL), jax.random.fold_in(key_of[4], 1), 0, N_COL - 1).astype(jnp.int32),
    }


def project(vectors, window):
    return lax.dot_general(vectors, window, (((0,), (0,)), ((), ())), precision=lax.Precision.HIGHEST, preferred_element_type=jnp.float32)


def reference(eigvec, reflectors, tfactors, offsets, owners):
    row_count = ORDER // N_ROW
    half_rows = WIN // 2
    matrix = jnp.concatenate([eigvec, jnp.zeros((half_rows, eigvec.shape[1]), eigvec.dtype)], 0)
    for turn_index in range(TICKS):
        def update_slab(matrix, slab_index):
            begin_row = (slab_index * row_count + offsets[turn_index, slab_index]).astype(jnp.int32)
            source = owners[turn_index, slab_index]
            vector_block = reflectors[slab_index, source]
            factor_block = tfactors[slab_index, source]
            window = lax.dynamic_slice_in_dim(matrix, begin_row, WIN, 0)
            coefficients = project(vector_block, window)
            scaled = jnp.dot(factor_block, coefficients, precision=lax.Precision.HIGHEST, preferred_element_type=jnp.float32)
            window = window - jnp.dot(vector_block, scaled, precision=lax.Precision.HIGHEST, preferred_element_type=jnp.float32)
            return lax.dynamic_update_slice_in_dim(matrix, window, begin_row, 0), None

        matrix, unused = lax.scan(update_slab, matrix, jnp.arange(N_ROW, dtype=jnp.int32))
    return matrix[:ORDER]
```

```python
import functools

import jax
import jax.numpy as jnp
from jax import lax
from jax.experimental import pallas as pl
from jax.experimental.pallas import tpu as pltpu
from jax.sharding import PartitionSpec as P

WIN = 1024
TICKS = 2
CHUNK = 256
PAD = 8
SUB = 8


def from_root(block, axis, owner):
    block = jnp.where(lax.axis_index(axis) == owner, block, jnp.zeros_like(block))
    return lax.psum(block, axis)


def from_behind(shard, axis, by):
    count = lax.axis_size(axis)
    pairs = [(i, i + by) for i in range(count) if 0 <= i + by < count]
    return lax.ppermute(shard, axis, pairs)


def positions(n):
    return lax.broadcasted_iota(jnp.int32, (n, n), 0), lax.broadcasted_iota(jnp.int32, (n, n), 1)


def fold(factor):
    half = factor.shape[0] // 2
    r, c = positions(half)
    first, side, second = factor[:half, :half], factor[:half, half:], factor[half:, half:]
    both = jnp.where(r <= c, first, second.T)
    diagonal = jnp.sum(jnp.where(r == c, second, 0.0), axis=0, keepdims=True)
    tail = jnp.pad(diagonal, ((0, PAD - 1), (0, half)))
    return jnp.concatenate([jnp.concatenate([both, side], 1), tail], 0)


def unfold(packed):
    half = packed.shape[1] // 2
    r, c = positions(half)
    both, side, diagonal = packed[:half, :half], packed[:half, half:], packed[half : half + 1, :half]
    first = jnp.where(r <= c, both, 0.0)
    second = jnp.where(r < c, both.T, jnp.where(r == c, jnp.broadcast_to(diagonal, both.shape), 0.0))
    return jnp.concatenate(
        [jnp.concatenate([first, side], 1), jnp.concatenate([jnp.zeros_like(first), second], 1)], 0
    )


def split(x):
    high = x.astype(jnp.bfloat16)
    return high, (x - high.astype(jnp.float32)).astype(jnp.bfloat16)


def product(left, right, dims):
    dot = functools.partial(
        lax.dot_general, dimension_numbers=(dims, ((), ())), preferred_element_type=jnp.float32
    )
    (lh, ll), (rh, rl) = left, right
    return dot(lh, rh) + (dot(lh, rl) + dot(ll, rh))


def tiles(x):
    return x.reshape(x.shape[0] // SUB, SUB, x.shape[1])


def rows_from(x, shift):
    turned = pltpu.roll(tiles(x), lax.rem(SUB - shift, SUB), axis=1)
    place = lax.broadcasted_iota(jnp.int32, turned[1:].shape, 1)
    return jnp.where(place + shift < SUB, turned[:-1], turned[1:]).reshape(x.shape[0] - SUB, x.shape[1])


def rows_at(x, shift):
    turned = pltpu.roll(tiles(x), shift, axis=1)
    none = jnp.zeros_like(turned[:1])
    ahead, behind = jnp.concatenate([turned, none], 0), jnp.concatenate([none, turned], 0)
    place = lax.broadcasted_iota(jnp.int32, ahead.shape, 1)
    return jnp.where(place >= shift, ahead, behind).reshape(x.shape[0] + SUB, x.shape[1])


def copy_kernel(x_ref, o_ref):
    o_ref[...] = x_ref[...]


def copy_middle(eigvec, begin, end):
    rows, cols = eigvec.shape
    step = WIN // 2
    return pl.pallas_call(
        copy_kernel,
        grid=((end - begin) // step,),
        in_specs=[pl.BlockSpec((step, cols), lambda i: (i + begin // step, 0))],
        out_specs=pl.BlockSpec((step, cols), lambda i: (i + begin // step, 0)),
        out_shape=jax.ShapeDtypeStruct((rows, cols), jnp.float32),
        cost_estimate=pl.CostEstimate(flops=0, bytes_accessed=8 * (end - begin) * cols, transcendentals=0),
    )(eigvec)


def window_kernel(plan, va, vb, ta, tb, upper, lower, held, out, low_out, frame):
    frame[:WIN, :] = upper[...]
    end = WIN + lower.shape[0]
    frame[WIN:end, :] = lower[...]
    frame[end:, :] = jnp.zeros_like(frame[end:, :])
    for tick in range(TICKS):
        begin, second = plan[0, tick], plan[1, tick] > 0
        vectors = split(jnp.where(second, vb[...], va[...]))
        factor = split(unfold(jnp.where(second, tb[...], ta[...])))
        shift = lax.rem(begin, SUB)
        near = pl.ds(pl.multiple_of(begin - shift, SUB), WIN + SUB)
        window = rows_from(frame[near, :], shift)
        coefficients = product(vectors, split(window), ((0,), (0,)))
        scaled = product(factor, split(coefficients), ((1,), (0,)))
        frame[near, :] -= rows_at(product(vectors, split(scaled), ((1,), (0,))), shift)
    out[...] = frame[:WIN, :]
    low_out[...] = frame[WIN:end, :]


def apply_window(plan, va, vb, ta, tb, eigvec, lower, held, chunk, width):
    rows, cols = eigvec.shape
    half = WIN // 2
    last = rows // WIN - 1
    block = va.shape[1]
    full = lambda x: pl.BlockSpec(x.shape, lambda i: (0,) * x.ndim)
    return pl.pallas_call(
        window_kernel,
        grid=(1,),
        in_specs=[
            pl.BlockSpec(memory_space=pltpu.SMEM),
            full(va), full(vb), full(ta), full(tb),
            pl.BlockSpec((WIN, width), lambda i: (last, chunk)),
            pl.BlockSpec((half, width), lambda i: (0, chunk)),
            pl.BlockSpec(memory_space=pl.ANY),
        ],
        out_specs=[
            pl.BlockSpec((WIN, width), lambda i: (last, chunk)),
            pl.BlockSpec((half, width), lambda i: (0, 0)),
        ],
        out_shape=[
            jax.ShapeDtypeStruct((rows, cols), jnp.float32),
            jax.ShapeDtypeStruct((half, width), jnp.float32),
        ],
        scratch_shapes=[pltpu.VMEM((WIN + half + SUB, width), jnp.float32)],
        input_output_aliases={7: 0},
        cost_estimate=pl.CostEstimate(
            flops=3 * TICKS * 2 * width * block * (2 * WIN + block),
            bytes_accessed=4 * (2 * WIN * block + 4 * WIN * width),
            transcendentals=0,
        ),
    )(plan, va, vb, ta, tb, eigvec, lower, held)


def per_device(eigvec, reflectors, tfactors, offsets, owners):
    rows, cols = eigvec.shape
    half = WIN // 2
    width = min(CHUNK, cols)
    own_row, own_col = lax.axis_index("row"), lax.axis_index("col")
    holders = lax.axis_size("col")
    vectors, factor = reflectors[0, 0], tfactors[0, 0]
    packed = fold(factor)
    source = lax.dynamic_slice_in_dim(owners, own_row, 1, 1)[:, 0]
    begin = lax.dynamic_slice_in_dim(offsets, own_row, 1, 1)[:, 0] - (rows - WIN)
    if holders == 2:
        swap = [(0, 1), (1, 0)]
        va, vb = vectors, lax.ppermute(vectors, "col", swap)
        ta, tb = packed, lax.ppermute(packed, "col", swap)
        second = (source != own_col).astype(jnp.int32)
    else:
        va, vb = (from_root(vectors, "col", source[t]) for t in range(TICKS))
        ta, tb = (from_root(packed, "col", source[t]) for t in range(TICKS))
        second = jnp.arange(TICKS, dtype=jnp.int32)
    plan = jnp.stack([begin, second])
    lower = from_behind(eigvec[:half], "row", -1)
    result = copy_middle(eigvec, half, rows - WIN)
    tops = []
    for chunk in range(cols // width):
        result, low = apply_window(plan, va, vb, ta, tb, eigvec, lower, result, chunk, width)
        tops.append(from_behind(low, "row", 1))
    for chunk, top in enumerate(tops):
        at = chunk * width
        top = jnp.where(own_row > 0, top, eigvec[:half, at : at + width])
        result = lax.dynamic_update_slice(result, top, (0, at))
    return result


def solution(mesh):
    return jax.shard_map(
        per_device,
        mesh=mesh,
        in_specs=(
            P("row", "col"),
            P("row", "col", None, None),
            P("row", "col", None, None),
            P(),
            P(),
        ),
        out_specs=P("row", "col"),
        check_vma=False,
    )
```

```python
import functools

import jax
import jax.numpy as jnp
from jax import lax
from jax.experimental import pallas as pl
from jax.experimental.pallas import tpu as pltpu
from jax.sharding import PartitionSpec as P

WIN = 1024
TICKS = 2
CHUNK = 256
PAD = 8
SUB = 8
LARGE = 56


def from_root(block, axis, owner):
    block = jnp.where(lax.axis_index(axis) == owner, block, jnp.zeros_like(block))
    return lax.psum(block, axis)


def from_behind(shard, axis, by):
    count = lax.axis_size(axis)
    pairs = [(i, i + by) for i in range(count) if 0 <= i + by < count]
    return lax.ppermute(shard, axis, pairs)


def positions(n):
    return lax.broadcasted_iota(jnp.int32, (n, n), 0), lax.broadcasted_iota(jnp.int32, (n, n), 1)


def fold(factor):
    half = factor.shape[0] // 2
    r, c = positions(half)
    first, side, second = factor[:half, :half], factor[:half, half:], factor[half:, half:]
    both = jnp.where(r <= c, first, second.T)
    diagonal = jnp.sum(jnp.where(r == c, second, 0.0), axis=0, keepdims=True)
    tail = jnp.pad(diagonal, ((0, PAD - 1), (0, half)))
    return jnp.concatenate([jnp.concatenate([both, side], 1), tail], 0)


def unfold(packed):
    half = packed.shape[1] // 2
    r, c = positions(half)
    both, side, diagonal = packed[:half, :half], packed[:half, half:], packed[half : half + 1, :half]
    first = jnp.where(r <= c, both, 0.0)
    second = jnp.where(r < c, both.T, jnp.where(r == c, jnp.broadcast_to(diagonal, both.shape), 0.0))
    return jnp.concatenate(
        [jnp.concatenate([first, side], 1), jnp.concatenate([jnp.zeros_like(first), second], 1)], 0
    )


def split(x):
    high = x.astype(jnp.bfloat16)
    return high, (x - high.astype(jnp.float32)).astype(jnp.bfloat16)


def product(left, right):
    (lh, ll), (rh, rl) = left, right
    return jnp.dot(
        jnp.concatenate([lh, lh, ll], 1),
        jnp.concatenate([rh, rl, rh], 0),
        preferred_element_type=jnp.float32,
    )


def tiles(x):
    return x.reshape(x.shape[0] // SUB, SUB, x.shape[1])


def rows_from(x, shift):
    turned = pltpu.roll(tiles(x), lax.rem(SUB - shift, SUB), axis=1)
    place = lax.broadcasted_iota(jnp.int32, turned[1:].shape, 1)
    return jnp.where(place + shift < SUB, turned[:-1], turned[1:]).reshape(x.shape[0] - SUB, x.shape[1])


def rows_at(x, shift):
    turned = pltpu.roll(tiles(x), shift, axis=1)
    none = jnp.zeros_like(turned[:1])
    ahead, behind = jnp.concatenate([turned, none], 0), jnp.concatenate([none, turned], 0)
    place = lax.broadcasted_iota(jnp.int32, ahead.shape, 1)
    return jnp.where(place >= shift, ahead, behind).reshape(x.shape[0] + SUB, x.shape[1])


def copy_kernel(width, x_ref, held, head, *uppers):
    step = x_ref.shape[0]
    at = pl.program_id(0)
    first = pl.num_programs(0) - WIN // step
    held[...] = x_ref[...]

    @pl.when(at == 0)
    def _():
        head[...] = x_ref[...]

    for part in range(WIN // step):

        @pl.when(at == first + part)
        def _():
            for chunk, upper in enumerate(uppers):
                upper[part * step : (part + 1) * step, :] = x_ref[:, chunk * width : (chunk + 1) * width]


def cost(flops, values):
    return pl.CostEstimate(flops=flops, bytes_accessed=4 * values, transcendentals=0)


def grant(mib):
    return pltpu.CompilerParams(vmem_limit_bytes=mib * 2**20)


def whole(shape):
    return pl.BlockSpec(shape, lambda i: (0,) * len(shape))


def copy_slab(eigvec, half, width):
    rows, cols = eigvec.shape
    count = cols // width
    rolling = pl.BlockSpec((half, cols), lambda i: (i, 0))
    return pl.pallas_call(
        functools.partial(copy_kernel, width),
        grid=(rows // half,),
        in_specs=[rolling],
        out_specs=[rolling, whole((half, cols))] + [whole((WIN, width))] * count,
        out_shape=[jax.ShapeDtypeStruct(eigvec.shape, jnp.float32), jax.ShapeDtypeStruct((half, cols), jnp.float32)]
        + [jax.ShapeDtypeStruct((WIN, width), jnp.float32)] * count,
        cost_estimate=cost(0, (2 * rows + half + WIN) * cols),
        compiler_params=grant(LARGE),
    )(eigvec)


def window_kernel(plan, va, vb, ta, tb, upper, lower, up_out, low_out, frame):
    end = WIN + lower.shape[0]
    frame[:WIN, :] = upper[...]
    frame[WIN:end, :] = lower[...]
    frame[end:, :] = jnp.zeros_like(frame[end:, :])
    for tick in range(TICKS):
        begin, second = plan[0, tick], plan[1, tick] > 0
        block = jnp.where(second, vb[...], va[...])
        vectors = split(block)
        factor = split(unfold(jnp.where(second, tb[...], ta[...])))
        shift = lax.rem(begin, SUB)
        near = pl.ds(pl.multiple_of(begin - shift, SUB), WIN + SUB)
        window = rows_from(frame[near, :], shift)
        coefficients = product(split(block.T), split(window))
        scaled = product(factor, split(coefficients))
        frame[near, :] -= rows_at(product(vectors, split(scaled)), shift)
    up_out[...] = frame[:WIN, :]
    low_out[...] = frame[WIN:end, :]


def apply_window(plan, va, vb, ta, tb, upper, lower, chunk):
    width = upper.shape[1]
    low = lower.shape[0]
    block = va.shape[1]
    return pl.pallas_call(
        window_kernel,
        grid=(1,),
        in_specs=[pl.BlockSpec(memory_space=pltpu.SMEM)] + [whole(x.shape) for x in (va, vb, ta, tb, upper)]
        + [pl.BlockSpec((low, width), lambda i: (0, chunk))],
        out_specs=[whole((WIN, width)), whole((low, width))],
        out_shape=[
            jax.ShapeDtypeStruct((WIN, width), jnp.float32),
            jax.ShapeDtypeStruct((low, width), jnp.float32),
        ],
        scratch_shapes=[pltpu.VMEM((WIN + low + SUB, width), jnp.float32)],
        cost_estimate=cost(3 * TICKS * 2 * width * block * (2 * WIN + block), 2 * WIN * block + 4 * WIN * width),
        compiler_params=grant(60),
    )(plan, va, vb, ta, tb, upper, lower)


def store_kernel(*refs):
    *parts, held, out = refs
    for chunk, part in enumerate(parts):
        width = part.shape[1]
        out[:, chunk * width : (chunk + 1) * width] = part[...]


def store_upper(parts, held):
    rows, cols = held.shape
    return pl.pallas_call(
        store_kernel,
        grid=(1,),
        in_specs=[whole(part.shape) for part in parts] + [pl.BlockSpec(memory_space=pltpu.HBM)],
        out_specs=pl.BlockSpec((WIN, cols), lambda i: (rows // WIN - 1, 0)),
        out_shape=jax.ShapeDtypeStruct(held.shape, jnp.float32),
        input_output_aliases={len(parts): 0},
        cost_estimate=cost(0, 2 * WIN * cols),
        compiler_params=grant(12),
    )(*parts, held)


def top_kernel(first, top, head, held, out):
    out[...] = jnp.where(first[0] > 0, head[...], top[...])


def store_top(first, top, head, held, chunk):
    half, width = top.shape
    return pl.pallas_call(
        top_kernel,
        grid=(1,),
        in_specs=[
            pl.BlockSpec(memory_space=pltpu.SMEM),
            whole(top.shape),
            pl.BlockSpec((half, width), lambda i: (0, chunk)),
            pl.BlockSpec(memory_space=pltpu.HBM),
        ],
        out_specs=pl.BlockSpec((half, width), lambda i: (0, chunk)),
        out_shape=jax.ShapeDtypeStruct(held.shape, jnp.float32),
        input_output_aliases={3: 0},
        cost_estimate=cost(0, 3 * half * width),
        compiler_params=grant(4),
    )(first, top, head, held)


def per_device(eigvec, reflectors, tfactors, offsets, owners):
    rows, cols = eigvec.shape
    half = WIN // 2
    width = min(CHUNK, cols)
    own_row, own_col = lax.axis_index("row"), lax.axis_index("col")
    holders = lax.axis_size("col")
    vectors, factor = reflectors[0, 0], tfactors[0, 0]
    packed = fold(factor)
    source = lax.dynamic_slice_in_dim(owners, own_row, 1, 1)[:, 0]
    begin = lax.dynamic_slice_in_dim(offsets, own_row, 1, 1)[:, 0] - (rows - WIN)
    if holders == 2:
        swap = [(0, 1), (1, 0)]
        va, vb = vectors, lax.ppermute(vectors, "col", swap)
        ta, tb = packed, lax.ppermute(packed, "col", swap)
        second = (source != own_col).astype(jnp.int32)
    else:
        va, vb = (from_root(vectors, "col", source[t]) for t in range(TICKS))
        ta, tb = (from_root(packed, "col", source[t]) for t in range(TICKS))
        second = jnp.arange(TICKS, dtype=jnp.int32)
    plan = jnp.stack([begin, second])
    result, head, *uppers = copy_slab(eigvec, half, width)
    lower = from_behind(head, "row", -1)
    parts, tops = [], []
    for chunk, upper in enumerate(uppers):
        part, low = apply_window(plan, va, vb, ta, tb, upper, lower, chunk)
        parts.append(part)
        tops.append(from_behind(low, "row", 1))
    result = store_upper(parts, result)
    first = (own_row == 0).astype(jnp.int32)[None]
    for chunk, top in enumerate(tops):
        result = store_top(first, top, head, result, chunk)
    return result


def solution(mesh):
    return jax.shard_map(
        per_device,
        mesh=mesh,
        in_specs=(
            P("row", "col"),
            P("row", "col", None, None),
            P("row", "col", None, None),
            P(),
            P(),
        ),
        out_specs=P("row", "col"),
        check_vma=False,
    )
```
